32 devices in a mesh: dp: 8 (over y, x, core), mp: 4 (over z).
Axes of the slice: x: 2, y: 2, z: 4, core: 2. Of those that a mesh axis runs over, the one named last changes fastest.
Arguments:
- slab_values: bfloat16 [32, 32, 2048], P(('dp', 'mp')), may hold values from -6 to 6
- row_ids: int32 [32, 32, 32], P(('dp', 'mp')), may hold values from 0 to 4095, as said below
- peer_counts: int32 [32, 32], P(('dp', 'mp')), may hold values from 1 to 32, as said below
- lookup_slots: int32 [8192, 16], P(('dp', 'mp')), may hold values from 0 to 1023, as said below
- labels: int32 [8192], P('dp'), may hold values 0 or 1
- sample_weight: float32 [8192], P('dp'), may hold values from 0.3 to 9
- weight_in: bfloat16 [1024, 8192], P(None, 'mp'), may hold values from -0.1875 to 0.1875
- bias_in: float32 [8192], P('mp'), may hold values from -3 to 3
- weight_out: bfloat16 [8192], P('mp'), may hold values from -0.0625 to 0.0625
- dense_accum: float32 [1024, 8192], P('dp', 'mp'), may hold values from 1e-08 to 1e-06
- table_rows: float32 [131072, 64], P(('dp', 'mp')), may hold values from -0.12 to 0.12
- table_accum: float32 [131072], P(('dp', 'mp')), may hold values from 1e-12 to 1e-05
Outputs:
- weight_new: bfloat16 [1024, 8192], P(None, 'mp')
- accum_new: float32 [1024, 8192], P('dp', 'mp')
- table_new: float32 [131072, 64], P(('dp', 'mp'))
- table_accum_new: float32 [131072], P(('dp', 'mp'))
The draws below stay inside these ranges and needn't reach their ends.
Inputs may be any that keep to these rules, and one draw needn't show every extreme that they name: `row_ids`: the first peer_counts entries of each device's list for an owner are distinct rows of that owner's shard. `peer_counts`: some owner has 32 touched rows on every device, and some device has 32 touched rows of every owner. `lookup_slots`: below the sum of that device's peer_counts; every device has a lookup of its last touched row.
All inputs are finite; a program needn't handle non-finite values. No bound on the sum of `labels` on one device may be relied on, other than what follows from the above.
Results may differ from the reference program's by a relative error of at most 0.0034.
Values may be sent and summed in bfloat16 or wider, within the bound.
A program may use at most 128 MiB of HBM per device.

```python
import math
import jax
import jax.numpy as jnp
from jax import lax

D_EMB = 64
NF = 16
H = 8192
B_DEV = 256
CAP = 32
ROWS_OWN = 4096
K = 1024
PEERS = 32
SAMPLES = 8192
TABLE_ROWS = 131072
N_DP = 8
N_MP = 4


def count_table(key):
    base = jax.random.fold_in(key, 7)
    counts = jax.random.randint(jax.random.fold_in(base, 1), (PEERS, PEERS), max(1, CAP // 4), CAP + 1)
    hot_owner = jax.random.randint(jax.random.fold_in(base, 2), (), 0, PEERS)
    full_device = jax.random.randint(jax.random.fold_in(base, 3), (), 0, PEERS)
    column = jnp.arange(PEERS)[None, :]
    row_number = jnp.arange(PEERS)[:, None]
    counts = jnp.where(column == hot_owner, CAP, counts)
    counts = jnp.where(row_number == full_device, CAP, counts)
    return counts.astype(jnp.int32)


def draw_peer_counts(key, part):
    return count_table(key)


def draw_lookup_slots(key, part):
    counts = count_table(key)
    live = jnp.sum(counts, axis=1)
    raw_draw = jax.random.randint(jax.random.fold_in(key, 11), (SAMPLES, NF), 0, 2 ** 30)
    device = jnp.arange(SAMPLES) // B_DEV
    within = jnp.arange(SAMPLES) % B_DEV
    drawn = raw_draw % live[device][:, None]
    chosen_sample = jax.random.randint(jax.random.fold_in(key, 19), (PEERS,), 0, B_DEV)
    chosen_feature = jax.random.randint(jax.random.fold_in(key, 23), (PEERS,), 0, NF)
    marked = (within == chosen_sample[device])[:, None] & (jnp.arange(NF)[None, :] == chosen_feature[device][:, None])
    return jnp.where(marked, live[device][:, None] - 1, drawn).astype(jnp.int32)


def draw_row_ids(key, part):
    stride = ROWS_OWN // CAP
    offsets = jax.random.randint(jax.random.fold_in(key, 13), (PEERS, PEERS, CAP), 0, stride)
    return (jnp.arange(CAP)[None, None, :] * stride + offsets).astype(jnp.int32)


def draw_sample_weight(key, part):
    position = jnp.arange(SAMPLES).astype(jnp.float32) / SAMPLES
    rising = 1.0 + 2.0 * position
    level = jax.random.uniform(jax.random.fold_in(key, 17), (SAMPLES,), jnp.float32, 0.5, 1.5)
    return (rising * level).astype(jnp.float32)


def with_ends(values, own_key, low, largest):
    spot = [jax.random.randint(jax.random.fold_in(own_key, axis), (), 0, length) for axis, length in enumerate(values.shape)]
    longest = values.shape.index(max(values.shape))
    beside = spot[:longest] + [(spot[longest] + 1) % values.shape[longest]] + spot[longest + 1:]
    return values.at[tuple(spot)].set(low).at[tuple(beside)].set(largest)


def shard_levels(key, dims, split, smallest, high):
    level = 1.0
    for dim, blocks in split:
        steps = jax.random.uniform(jax.random.fold_in(jax.random.fold_in(key, 6), dim), (blocks,), jnp.float32, smallest / len(split), high / len(split))
        level = level * jnp.repeat(jnp.exp(steps), dims[dim] // blocks).reshape((-1,) + (1,) * (len(dims) - 1 - dim))
    return level


def gaussian(key, extent, deviation, reach, split=(), kind=jnp.bfloat16):
    loudness = shard_levels(key, extent, split, -0.22, 0.18) if split else 1.0
    result = jax.random.normal(key, extent, jnp.float32) * deviation * loudness
    return jnp.minimum(jnp.maximum(result, -reach), reach).astype(kind)


def setup_inputs(seed: int = 0) -> dict:
    seeds = jax.random.split(jax.random.key(seed), 13)
    return {
        "slab_values": gaussian(seeds[0], (PEERS, PEERS, CAP * D_EMB), 1.0, 6.0, ((0, 32),)),
        "row_ids": draw_row_ids(jax.random.fold_in(seeds[12], 71), 0),
        "peer_counts": draw_peer_counts(jax.random.fold_in(seeds[12], 71), 0),
        "lookup_slots": draw_lookup_slots(jax.random.fold_in(seeds[12], 71), 0),
        "labels": with_ends((jax.random.randint(seeds[4], (SAMPLES,), 0, 4) < 1).astype(jnp.int32), jax.random.fold_in(seeds[4], 1), 0, 1),
        "sample_weight": draw_sample_weight(jax.random.fold_in(seeds[12], 71), 0),
        "weight_in": gaussian(seeds[6], (K, H), K ** -0.5, 0.1875, ((1, 4),)),
        "bias_in": gaussian(seeds[7], (H,), 0.5, 3.0, ((0, 4),), jnp.float32),
        "weight_out": gaussian(seeds[8], (H,), H ** -0.5, 0.0625, ((0, 4),)),
        "dense_accum": jnp.clip(jnp.exp(math.log(9.999999974752427e-07) - 4.6051702 * jax.random.uniform(seeds[9], (K, H), jnp.float32) ** shard_levels(seeds[9], (K, H), ((0, 8), (1, 4)), -0.2, 0.2)), 9.99999993922529e-09, 9.999999974752427e-07),
        "table_rows": gaussian(seeds[10], (TABLE_ROWS, D_EMB), 0.02, 0.12, ((0, 32),), jnp.float32),
        "table_accum": jnp.clip(jnp.exp(math.log(9.999999747378752e-06) - 16.118096 * jax.random.uniform(seeds[11], (TABLE_ROWS,), jnp.float32) ** shard_levels(seeds[11], (TABLE_ROWS,), ((0, 32),), -0.2, 0.2)), 9.999999960041972e-13, 9.999999747378752e-06),
    }


clip_norm = 1.0
dense_rate = 0.02
table_rate = 0.5
adagrad_eps = 1e-10

def slot_index(compact, counts, capacity):
    slot_ends = jnp.cumsum(counts)
    owner_index = lax.optimization_barrier(jnp.sum((compact[..., None] >= slot_ends).astype(jnp.int32), axis=-1))
    slot_starts = slot_ends - counts
    owner_match = owner_index[..., None] == jnp.arange(counts.shape[0], dtype=jnp.int32)
    owner_begin = lax.optimization_barrier(jnp.sum(jnp.where(owner_match, slot_starts, 0), axis=-1))
    return (owner_index * capacity + compact - owner_begin).astype(jnp.int32)

def reference(slab_values, row_ids, peer_counts, lookup_slots, labels, sample_weight, weight_in, bias_in, weight_out, dense_accum, table_rows, table_accum):
    group_rows = N_MP * B_DEV
    slabs = slab_values.reshape(N_DP, N_MP, PEERS * CAP, D_EMB)
    counts = peer_counts.reshape(N_DP, N_MP, PEERS)
    slots = lookup_slots.reshape(N_DP, N_MP, B_DEV, NF)
    targets = labels.astype(jnp.float32).reshape(N_DP, group_rows)
    weights = sample_weight.reshape(N_DP, group_rows)

    def group_step(carry, inputs):
        grad_in, grad_bias, grad_out = carry
        slab, count, slot, target, weight = inputs

        def pool(one_slab, one_count, one_slot):
            index = slot_index(one_slot, one_count, CAP)
            return (one_slab[index].reshape(B_DEV, K), index)
        pooled, index = jax.vmap(pool)(slab, count, slot)
        pooled = pooled.reshape(group_rows, K)
        act = jnp.dot(pooled, weight_in, preferred_element_type=jnp.float32) + bias_in
        hidden = jax.nn.silu(act).astype(jnp.bfloat16)
        logit = jnp.dot(hidden, weight_out, preferred_element_type=jnp.float32)
        dlogit = weight * (jax.nn.sigmoid(logit) - target)
        sigma = jax.nn.sigmoid(act)
        dact = (dlogit[:, None] * weight_out.astype(jnp.float32)[None, :] * sigma * (1.0 + act * (1.0 - sigma))).astype(jnp.bfloat16)
        grad_in = grad_in + lax.dot_general(pooled, dact, (((0,), (0,)), ((), ())), preferred_element_type=jnp.float32)
        grad_bias = grad_bias + lax.optimization_barrier(jnp.sum(dact.astype(jnp.float32), axis=0))
        grad_out = grad_out + jnp.dot(dlogit, hidden.astype(jnp.float32), precision=lax.Precision.HIGHEST)
        dpooled = lax.dot_general(dact, weight_in, (((1,), (1,)), ((), ())), preferred_element_type=jnp.float32)
        pieces = dpooled.reshape(N_MP, B_DEV * NF, D_EMB)

        def gather_slots(piece, one_index):
            return jax.ops.segment_sum(piece, one_index.reshape(-1), num_segments=PEERS * CAP)
        slot_grad = jax.vmap(gather_slots)(pieces, index)
        return ((grad_in, grad_bias, grad_out), slot_grad)
    start = (jnp.zeros((K, H), jnp.float32), jnp.zeros((H,), jnp.float32), jnp.zeros((H,), jnp.float32))
    (grad_in, grad_bias, grad_out), slot_grad = lax.scan(group_step, start, (slabs, counts, slots, targets, weights))
    slot_grad = slot_grad.reshape(PEERS, PEERS * CAP, D_EMB)
    total = jnp.sum(grad_in * grad_in) + jnp.sum(grad_bias * grad_bias) + jnp.sum(grad_out * grad_out) + jnp.sum(slot_grad * slot_grad)
    scale = clip_norm / jnp.maximum(jnp.sqrt(total), clip_norm)
    clipped = scale * grad_in
    accum_new = dense_accum + clipped * clipped
    weight_new = (weight_in.astype(jnp.float32) - dense_rate * clipped / (jnp.sqrt(accum_new) + adagrad_eps)).astype(jnp.bfloat16)
    owners = jnp.arange(PEERS, dtype=jnp.int32)[None, :, None]
    global_rows = (owners * ROWS_OWN + row_ids).reshape(-1)
    received = scale * jax.ops.segment_sum(slot_grad.reshape(-1, D_EMB), global_rows, num_segments=TABLE_ROWS)
    table_accum_new = table_accum + lax.optimization_barrier(jnp.mean(received * received, axis=1))
    table_new = table_rows - table_rate * received / (jnp.sqrt(table_accum_new)[:, None] + adagrad_eps)
    return (weight_new, accum_new, table_new, table_accum_new)
```

```python
import functools

import jax
import jax.numpy as jnp
from jax import lax
from jax.experimental import pallas as pl
from jax.experimental.pallas import tpu as pltpu
from jax.sharding import PartitionSpec as P

clip_norm = 1.0
dense_rate = 0.02
table_rate = 0.5
adagrad_eps = 1e-10
MESH = pl.DeviceIdType.MESH
VMEM_BYTES = 60 * 1024 * 1024


def slot_index(compact, counts, capacity):
    slot_ends = jnp.cumsum(counts)
    owner_index = jnp.sum((compact[..., None] >= slot_ends).astype(jnp.int32), axis=-1)
    slot_starts = slot_ends - counts
    owner_match = owner_index[..., None] == jnp.arange(counts.shape[0], dtype=jnp.int32)
    owner_begin = jnp.sum(jnp.where(owner_match, slot_starts, 0), axis=-1)
    return owner_index * capacity + compact - owner_begin


def flat_place(axes, sizes):
    place = jnp.int32(0)
    for axis, size in zip(axes, sizes):
        place = place * size + lax.axis_index(axis)
    return place


def device_of(axes, sizes, place):
    where = {}
    for axis, size in reversed(list(zip(axes, sizes))):
        where[axis] = lax.rem(place, size)
        place = lax.div(place, size)
    return where


def greet(axes, sizes, me, number):
    barrier = pltpu.get_barrier_semaphore()
    for step in range(1, number):
        peer = lax.rem(me + step, number)
        pl.semaphore_signal(
            barrier, inc=1, device_id=device_of(axes, sizes, peer), device_id_type=MESH
        )
    pl.semaphore_wait(barrier, number - 1)


def exchange_kernel(axes, sizes, splits, *refs):
    count = len(splits)
    ins, outs = refs[:count], refs[count : 2 * count]
    send_sem, recv_sem = refs[2 * count :]
    number = 1
    for size in sizes:
        number *= size
    me = flat_place(axes, sizes)
    greet(axes, sizes, me, number)
    copies = []
    for step in range(1, number):
        peer = lax.rem(me + step, number)
        for i, split in enumerate(splits):
            copy = pltpu.make_async_remote_copy(
                src_ref=ins[i].at[peer] if split else ins[i],
                dst_ref=outs[i].at[me],
                send_sem=send_sem.at[i, step],
                recv_sem=recv_sem.at[i, step],
                device_id=device_of(axes, sizes, peer),
                device_id_type=MESH,
            )
            copy.start()
            copies.append(copy)
    for i, split in enumerate(splits):
        outs[i][me] = ins[i][me] if split else ins[i][...]
    for copy in copies:
        copy.wait()


def exchange(mesh, axes, arrays, splits, collective_id):
    sizes = tuple(mesh.shape[axis] for axis in axes)
    number = 1
    for size in sizes:
        number *= size
    shapes = [
        jax.ShapeDtypeStruct(a.shape if s else (number,) + a.shape, a.dtype)
        for a, s in zip(arrays, splits)
    ]
    return pl.pallas_call(
        functools.partial(exchange_kernel, axes, sizes, splits),
        out_shape=shapes,
        in_specs=[pl.BlockSpec(memory_space=pltpu.VMEM)] * len(arrays),
        out_specs=[pl.BlockSpec(memory_space=pltpu.VMEM)] * len(arrays),
        scratch_shapes=[
            pltpu.SemaphoreType.DMA((len(arrays), number)),
            pltpu.SemaphoreType.DMA((len(arrays), number)),
        ],
        compiler_params=pltpu.CompilerParams(collective_id=collective_id, has_side_effects=True),
    )(*arrays)


def bit_orders(number):
    bits = list(range(number.bit_length() - 1))
    return (bits, bits[:1] + bits[:0:-1])


def subsets(bits):
    if not bits:
        return [[]]
    rest = subsets(bits[1:])
    return rest + [[bits[0]] + r for r in rest]


def flip(place, bit):
    step = 1 << bit
    return place + step * (1 - 2 * lax.rem(lax.div(place, step), 2))


def flip_all(place, bits):
    for bit in bits:
        place = flip(place, bit)
    return place


def scatter_kernel(number, grad_ref, small_ref, out_ref, gathered_ref, *scratch):
    orders = bit_orders(number)
    phases = len(orders[0])
    gots = (scratch[:phases], scratch[phases : 2 * phases])
    sums = (scratch[2 * phases : 3 * phases - 1], scratch[3 * phases - 1 : 4 * phases - 2])
    send_sem, recv_sem, small_send, small_recv = scratch[4 * phases - 2 :]
    me = lax.axis_index("dp")
    half = out_ref.shape[0] // 2
    greet(("dp",), (number,), me, number)
    flying = [[], []]
    everything = []

    def start(phase, stream):
        order = orders[stream]
        bit, left = order[phase], order[phase + 1 :]
        kept = subsets(left)
        flying[stream] = []
        for slot, subset in enumerate(kept):
            if phase == 0:
                block = flip(flip_all(me, subset), bit)
                source = grad_ref.at[block, pl.ds(stream * half, half)]
            else:
                source = sums[stream][phase - 1].at[len(kept) + slot]
            copy = pltpu.make_async_remote_copy(
                src_ref=source,
                dst_ref=gots[stream][phase].at[slot],
                send_sem=send_sem.at[stream, phase, slot],
                recv_sem=recv_sem.at[stream, phase, slot],
                device_id={"dp": flip(me, bit)},
                device_id_type=MESH,
            )
            copy.start()
            flying[stream].append(copy)
            everything.append(copy)

    def add(phase, stream):
        kept = subsets(orders[stream][phase + 1 :])
        for slot, subset in enumerate(kept):
            block = flip_all(me, subset)

            def step(i, carry):
                rows = pl.ds(pl.multiple_of(i * 16, 16), 16)
                if phase == 0:
                    begin = pl.multiple_of(stream * half + i * 16, 16)
                    mine = grad_ref[block, pl.ds(begin, 16)]
                else:
                    mine = sums[stream][phase - 1][slot, rows]
                came = gots[stream][phase][slot, rows]
                total = mine.astype(jnp.float32) + came.astype(jnp.float32)
                if phase == phases - 1:
                    out_ref[pl.ds(pl.multiple_of(stream * half + i * 16, 16), 16)] = total
                else:
                    sums[stream][phase][slot, rows] = total.astype(jnp.bfloat16)
                return carry

            lax.fori_loop(0, half // 16, step, 0)

    start(0, 0)
    start(0, 1)
    smalls = []
    for step in range(1, number):
        peer = lax.rem(me + step, number)
        copy = pltpu.make_async_remote_copy(
            src_ref=small_ref,
            dst_ref=gathered_ref.at[me],
            send_sem=small_send.at[step],
            recv_sem=small_recv.at[step],
            device_id={"dp": peer},
            device_id_type=MESH,
        )
        copy.start()
        smalls.append(copy)
    gathered_ref[me] = small_ref[...]
    for phase in range(phases):
        for stream in range(2):
            for copy in flying[stream]:
                copy.wait_recv()
            add(phase, stream)
            if phase < phases - 1:
                start(phase + 1, stream)
    for copy in everything:
        copy.wait_send()
    for copy in smalls:
        copy.wait()


def scatter_grad(mesh, grad, small, collective_id):
    number = mesh.shape["dp"]
    rows, width = grad.shape[0] // number, grad.shape[1]
    blocks = grad.reshape(number, rows, width)
    phases = number.bit_length() - 1
    gots = [
        pltpu.VMEM((number >> (phase + 1), rows // 2, width), jnp.bfloat16)
        for phase in range(phases)
    ]
    return pl.pallas_call(
        functools.partial(scatter_kernel, number),
        out_shape=[
            jax.ShapeDtypeStruct((rows, width), jnp.float32),
            jax.ShapeDtypeStruct((number,) + small.shape, small.dtype),
        ],
        in_specs=[pl.BlockSpec(memory_space=pltpu.VMEM)] * 2,
        out_specs=[pl.BlockSpec(memory_space=pltpu.VMEM)] * 2,
        scratch_shapes=gots
        + gots
        + gots[:-1]
        + gots[:-1]
        + [
            pltpu.SemaphoreType.DMA((2, phases, number // 2)),
            pltpu.SemaphoreType.DMA((2, phases, number // 2)),
            pltpu.SemaphoreType.DMA((number,)),
            pltpu.SemaphoreType.DMA((number,)),
        ],
        compiler_params=pltpu.CompilerParams(
            collective_id=collective_id, has_side_effects=True, vmem_limit_bytes=VMEM_BYTES
        ),
    )(blocks, small)


def gather_kernel(number, mine_ref, out_ref, local_sem, send_sem, recv_sem):
    me = lax.axis_index("dp")
    rows = mine_ref.shape[0]
    greet(("dp",), (number,), me, number)
    orders = [order[::-1] for order in bit_orders(number)]
    half = rows // 2
    local = pltpu.make_async_copy(mine_ref, out_ref.at[me], local_sem)
    local.start()
    copies = []
    held = [[[]], [[]]]
    slot = [0, 0]
    waiting = [[], []]
    for phase in range(len(orders[0])):
        for stream, order in enumerate(orders):
            bit = order[phase]
            part = pl.ds(stream * half, half)
            for copy in waiting[stream]:
                copy.wait_recv()
            waiting[stream] = []
            for subset in held[stream]:
                block = flip_all(me, subset)
                source = out_ref.at[block, part] if subset else mine_ref.at[part]
                copy = pltpu.make_async_remote_copy(
                    src_ref=source,
                    dst_ref=out_ref.at[block, part],
                    send_sem=send_sem.at[stream, slot[stream]],
                    recv_sem=recv_sem.at[stream, slot[stream]],
                    device_id={"dp": flip(me, bit)},
                    device_id_type=MESH,
                )
                copy.start()
                copies.append(copy)
                waiting[stream].append(copy)
                slot[stream] += 1
            held[stream] = held[stream] + [subset + [bit] for subset in held[stream]]
    for stream in range(2):
        for copy in waiting[stream]:
            copy.wait_recv()
    for copy in copies:
        copy.wait_send()
    local.wait()


def gather_weights(mesh, mine, collective_id):
    number = mesh.shape["dp"]
    out = pl.pallas_call(
        functools.partial(gather_kernel, number),
        out_shape=jax.ShapeDtypeStruct((number,) + mine.shape, mine.dtype),
        in_specs=[pl.BlockSpec(memory_space=pltpu.VMEM)],
        out_specs=pl.BlockSpec(memory_space=pltpu.VMEM),
        scratch_shapes=[
            pltpu.SemaphoreType.DMA,
            pltpu.SemaphoreType.DMA((2, number)),
            pltpu.SemaphoreType.DMA((2, number)),
        ],
        compiler_params=pltpu.CompilerParams(
            collective_id=collective_id, has_side_effects=True, vmem_limit_bytes=VMEM_BYTES
        ),
    )(mine)
    return out.reshape(number * mine.shape[0], mine.shape[1])


def pool_kernel(slab_ref, index_ref, out_ref):
    slab = slab_ref[0]
    pairs, lanes = slab.shape
    batch, features = index_ref.shape[1:]
    pair_number = lax.broadcasted_iota(jnp.int32, (batch, pairs), 1)
    low = lax.broadcasted_iota(jnp.int32, (batch, lanes), 1) < lanes // 2
    for first in range(0, features, 2):
        halves = []
        for side in range(2):
            column = index_ref[0, :, first + side : first + side + 1]
            hot = jnp.where((column >> 1) == pair_number, 1.0, 0.0).astype(jnp.bfloat16)
            found = jnp.dot(hot, slab, preferred_element_type=jnp.float32)
            turned = pltpu.roll(found, lanes // 2, 1)
            halves.append(jnp.where((column & 1) == side, found, turned))
        start = first // 2 * lanes
        out_ref[:, start : start + lanes] = jnp.where(low, halves[0], halves[1]).astype(
            jnp.bfloat16
        )


def pool(slabs, indices):
    groups, pairs, lanes = slabs.shape
    batch, features = indices.shape[1:]
    return pl.pallas_call(
        pool_kernel,
        grid=(groups,),
        out_shape=jax.ShapeDtypeStruct((groups * batch, features * lanes // 2), jnp.bfloat16),
        in_specs=[
            pl.BlockSpec((1, pairs, lanes), lambda g: (g, 0, 0)),
            pl.BlockSpec((1, batch, features), lambda g: (g, 0, 0)),
        ],
        out_specs=pl.BlockSpec((batch, features * lanes // 2), lambda g: (g, 0)),
        compiler_params=pltpu.CompilerParams(vmem_limit_bytes=VMEM_BYTES),
    )(slabs, indices)


def slot_kernel(dact_ref, weight_ref, index_ref, turned_ref, out_ref, hot_ref, value_ref):
    pairs, lanes = out_ref.shape[1:]
    batch, features = index_ref.shape[1:]
    dpooled = lax.dot_general(
        dact_ref[...], weight_ref[...], (((1,), (1,)), ((), ())), preferred_element_type=jnp.float32
    )
    pair_number = lax.broadcasted_iota(jnp.int32, (pairs, batch), 0)
    upper = (lax.broadcasted_iota(jnp.int32, (batch, lanes), 1) >= lanes // 2).astype(jnp.int32)
    for feature in range(features):
        start = feature // 2 * lanes
        piece = dpooled[:, start : start + lanes]
        odd = index_ref[0, :, feature : feature + 1] & 1
        piece = jnp.where(odd == feature % 2, piece, pltpu.roll(piece, lanes // 2, 1))
        piece = jnp.where(upper == odd, piece, 0.0)
        high = piece.astype(jnp.bfloat16)
        rows = pl.ds(feature * batch, batch)
        value_ref[rows, 0:lanes] = high
        value_ref[rows, lanes : 2 * lanes] = (piece - high.astype(jnp.float32)).astype(jnp.bfloat16)
        line = turned_ref[0, feature : feature + 1, :] >> 1
        hot_ref[:, rows] = jnp.where(line == pair_number, 1.0, 0.0).astype(jnp.bfloat16)
    both = jnp.dot(hot_ref[...], value_ref[...], preferred_element_type=jnp.float32)
    out_ref[0] = (both[:, :lanes] + both[:, lanes:]).astype(jnp.bfloat16)


def slot_grads(dact, weight, indices, turned, pairs):
    groups, batch, features = indices.shape
    inputs, hidden = weight.shape
    lanes = 2 * inputs // features
    return pl.pallas_call(
        slot_kernel,
        grid=(groups,),
        out_shape=jax.ShapeDtypeStruct((groups, pairs, lanes), jnp.bfloat16),
        in_specs=[
            pl.BlockSpec((batch, hidden), lambda g: (g, 0)),
            pl.BlockSpec((inputs, hidden), lambda g: (0, 0)),
            pl.BlockSpec((1, batch, features), lambda g: (g, 0, 0)),
            pl.BlockSpec((1, features, batch), lambda g: (g, 0, 0)),
        ],
        out_specs=pl.BlockSpec((1, pairs, lanes), lambda g: (g, 0, 0)),
        scratch_shapes=[
            pltpu.VMEM((pairs, features * batch), jnp.bfloat16),
            pltpu.VMEM((features * batch, 2 * lanes), jnp.bfloat16),
        ],
        compiler_params=pltpu.CompilerParams(vmem_limit_bytes=VMEM_BYTES),
    )(dact, weight, indices, turned)


def table_kernel(arrived_ref, even_ref, odd_ref, out_ref):
    rows, width = out_ref.shape
    arrived = arrived_ref[...]
    count = arrived.shape[0]
    number = lax.broadcasted_iota(jnp.int32, (rows, count), 0) + pl.program_id(0) * rows
    even = jnp.where(even_ref[...] == number, 1.0, 0.0).astype(jnp.bfloat16)
    odd = jnp.where(odd_ref[...] == number, 1.0, 0.0).astype(jnp.bfloat16)
    first = jnp.dot(even, arrived, preferred_element_type=jnp.float32)
    second = jnp.dot(odd, arrived, preferred_element_type=jnp.float32)
    out_ref[...] = (first + pltpu.roll(second, width, 1))[:, :width]


def table_sums(arrived, even, odd, rows):
    count, lanes = arrived.shape
    tile = 512
    return pl.pallas_call(
        table_kernel,
        grid=(rows // tile,),
        out_shape=jax.ShapeDtypeStruct((rows, lanes // 2), jnp.float32),
        in_specs=[
            pl.BlockSpec((count, lanes), lambda r: (0, 0)),
            pl.BlockSpec((1, count), lambda r: (0, 0)),
            pl.BlockSpec((1, count), lambda r: (0, 0)),
        ],
        out_specs=pl.BlockSpec((tile, lanes // 2), lambda r: (r, 0)),
    )(arrived, even, odd)


def body(
    mesh,
    slab_values,
    row_ids,
    peer_counts,
    lookup_slots,
    labels,
    sample_weight,
    weight_in,
    bias_in,
    weight_out,
    dense_accum,
    table_rows,
    table_accum,
):
    peers = peer_counts.shape[1]
    capacity = row_ids.shape[2]
    emb_width = slab_values.shape[2] // capacity
    lanes = 2 * emb_width
    pairs = peers * capacity // 2
    index = slot_index(lookup_slots, peer_counts[0], capacity)
    slabs, indices = exchange(
        mesh, ("mp",), (slab_values.reshape(pairs, lanes), index), (False, False), 0
    )
    turned = jnp.swapaxes(indices, 1, 2)
    group = pool(slabs, indices)
    act = jnp.dot(group, weight_in, preferred_element_type=jnp.float32) + bias_in
    hidden = jax.nn.silu(act).astype(jnp.bfloat16)
    logit_part = jnp.dot(hidden, weight_out, preferred_element_type=jnp.float32)
    (logit_parts,) = exchange(mesh, ("mp",), (logit_part.reshape(-1, 128),), (False,), 1)
    logit = jnp.sum(logit_parts, axis=0).reshape(-1)
    dlogit = sample_weight * (jax.nn.sigmoid(logit) - labels.astype(jnp.float32))
    sigma = jax.nn.sigmoid(act)
    dact = (
        dlogit[:, None]
        * weight_out.astype(jnp.float32)[None, :]
        * sigma
        * (1.0 + act * (1.0 - sigma))
    ).astype(jnp.bfloat16)
    grad_in = lax.dot_general(
        group, dact, (((0,), (0,)), ((), ())), preferred_element_type=jnp.float32
    ).astype(jnp.bfloat16)
    grad_bias = jnp.sum(dact.astype(jnp.float32), axis=0)
    grad_out = jnp.sum(dlogit[:, None] * hidden.astype(jnp.float32), axis=0)
    small = jnp.concatenate([grad_bias.reshape(-1, 128), grad_out.reshape(-1, 128)])
    grad_rows, smalls = scatter_grad(mesh, grad_in, small, 2)
    partial = slot_grads(dact, weight_in, indices, turned, pairs)
    (parts,) = exchange(mesh, ("mp",), (partial,), (True,), 3)
    slot_grad = jnp.sum(parts.astype(jnp.float32), axis=0)
    first_group = (lax.axis_index("dp") == 0).astype(jnp.float32)
    small_sum = jnp.sum(smalls, axis=0)
    square = (
        jnp.sum(grad_rows * grad_rows)
        + first_group * jnp.sum(small_sum * small_sum)
        + jnp.sum(slot_grad * slot_grad)
    )
    arrived, arrived_rows, squares = exchange(
        mesh,
        ("dp", "mp"),
        (
            slot_grad.astype(jnp.bfloat16).reshape(peers, capacity // 2, lanes),
            row_ids.reshape(peers, 1, capacity),
            jnp.full((8, 128), square, jnp.float32),
        ),
        (True, True, False),
        4,
    )
    total = jnp.sum(squares[:, 0, 0])
    scale = clip_norm / jnp.maximum(jnp.sqrt(total), clip_norm)
    own_rows = dense_accum.shape[0]
    row_start = lax.axis_index("dp") * own_rows
    clipped = scale * grad_rows
    accum_new = dense_accum + clipped * clipped
    weight_part = lax.dynamic_slice_in_dim(weight_in, row_start, own_rows, 0).astype(jnp.float32)
    updated = (weight_part - dense_rate * clipped / (jnp.sqrt(accum_new) + adagrad_eps)).astype(
        jnp.bfloat16
    )
    weight_new = gather_weights(mesh, updated, 5)
    flat_rows = arrived_rows.reshape(-1, 2)
    received = scale * table_sums(
        arrived.reshape(pairs, lanes),
        flat_rows[:, 0].reshape(1, -1),
        flat_rows[:, 1].reshape(1, -1),
        table_rows.shape[0],
    )
    table_accum_new = table_accum + jnp.mean(received * received, axis=1)
    table_new = table_rows - table_rate * received / (
        jnp.sqrt(table_accum_new)[:, None] + adagrad_eps
    )
    return (weight_new, accum_new, table_new, table_accum_new)


def solution(mesh):
    placed = (
        P(("dp", "mp"), None, None),
        P(("dp", "mp"), None, None),
        P(("dp", "mp"), None),
        P(("dp", "mp"), None),
        P("dp"),
        P("dp"),
        P(None, "mp"),
        P("mp"),
        P("mp"),
        P("dp", "mp"),
        P(("dp", "mp"), None),
        P(("dp", "mp")),
    )
    return jax.shard_map(
        functools.partial(body, mesh),
        mesh=mesh,
        in_specs=placed,
        out_specs=(P(None, "mp"), P("dp", "mp"), P(("dp", "mp"), None), P(("dp", "mp"))),
        check_vma=False,
    )
```

```python
import functools

import jax
import jax.numpy as jnp
from jax import lax
from jax.experimental import pallas as pl
from jax.experimental.pallas import tpu as pltpu
from jax.sharding import PartitionSpec as P

clip_norm = 1.0
dense_rate = 0.02
table_rate = 0.5
adagrad_eps = 1e-10
MESH = pl.DeviceIdType.MESH
VMEM_BYTES = 60 * 1024 * 1024


def slot_index(compact, counts, capacity):
    slot_ends = jnp.cumsum(counts)
    owner_index = jnp.sum((compact[..., None] >= slot_ends).astype(jnp.int32), axis=-1)
    slot_starts = slot_ends - counts
    owner_match = owner_index[..., None] == jnp.arange(counts.shape[0], dtype=jnp.int32)
    owner_begin = jnp.sum(jnp.where(owner_match, slot_starts, 0), axis=-1)
    return owner_index * capacity + compact - owner_begin


def flat_place(axes, sizes):
    place = jnp.int32(0)
    for axis, size in zip(axes, sizes):
        place = place * size + lax.axis_index(axis)
    return place


def device_of(axes, sizes, place):
    where = {}
    for axis, size in reversed(list(zip(axes, sizes))):
        where[axis] = lax.rem(place, size)
        place = lax.div(place, size)
    return where


def greet(axes, sizes, me, number):
    barrier = pltpu.get_barrier_semaphore()
    for step in range(1, number):
        peer = lax.rem(me + step, number)
        pl.semaphore_signal(
            barrier, inc=1, device_id=device_of(axes, sizes, peer), device_id_type=MESH
        )
    pl.semaphore_wait(barrier, number - 1)


def exchange_kernel(axes, sizes, splits, *refs):
    count = len(splits)
    ins, outs = refs[:count], refs[count : 2 * count]
    send_sem, recv_sem = refs[2 * count :]
    number = 1
    for size in sizes:
        number *= size
    me = flat_place(axes, sizes)
    greet(axes, sizes, me, number)
    copies = []
    for step in range(1, number):
        peer = lax.rem(me + step, number)
        for i, split in enumerate(splits):
            copy = pltpu.make_async_remote_copy(
                src_ref=ins[i].at[peer] if split else ins[i],
                dst_ref=outs[i].at[me],
                send_sem=send_sem.at[i, step],
                recv_sem=recv_sem.at[i, step],
                device_id=device_of(axes, sizes, peer),
                device_id_type=MESH,
            )
            copy.start()
            copies.append(copy)
    for i, split in enumerate(splits):
        outs[i][me] = ins[i][me] if split else ins[i][...]
    for copy in copies:
        copy.wait()


def exchange(mesh, axes, arrays, splits, collective_id):
    sizes = tuple(mesh.shape[axis] for axis in axes)
    number = 1
    for size in sizes:
        number *= size
    shapes = [
        jax.ShapeDtypeStruct(a.shape if s else (number,) + a.shape, a.dtype)
        for a, s in zip(arrays, splits)
    ]
    return pl.pallas_call(
        functools.partial(exchange_kernel, axes, sizes, splits),
        out_shape=shapes,
        in_specs=[pl.BlockSpec(memory_space=pltpu.VMEM)] * len(arrays),
        out_specs=[pl.BlockSpec(memory_space=pltpu.VMEM)] * len(arrays),
        scratch_shapes=[
            pltpu.SemaphoreType.DMA((len(arrays), number)),
            pltpu.SemaphoreType.DMA((len(arrays), number)),
        ],
        compiler_params=pltpu.CompilerParams(collective_id=collective_id, has_side_effects=True),
    )(*arrays)


def bit_orders(number):
    bits = list(range(number.bit_length() - 1))
    return (bits, bits[:1] + bits[:0:-1])


def subsets(bits):
    if not bits:
        return [[]]
    rest = subsets(bits[1:])
    return rest + [[bits[0]] + r for r in rest]


def flip(place, bit):
    step = 1 << bit
    return place + step * (1 - 2 * lax.rem(lax.div(place, step), 2))


def flip_all(place, bits):
    for bit in bits:
        place = flip(place, bit)
    return place


def scatter_kernel(number, grad_ref, small_ref, out_ref, gathered_ref, *scratch):
    orders = bit_orders(number)
    phases = len(orders[0])
    gots = (scratch[:phases], scratch[phases : 2 * phases])
    sums = (scratch[2 * phases : 3 * phases - 1], scratch[3 * phases - 1 : 4 * phases - 2])
    send_sem, recv_sem, small_send, small_recv = scratch[4 * phases - 2 :]
    me = lax.axis_index("dp")
    half = out_ref.shape[0] // 2
    greet(("dp",), (number,), me, number)
    flying = [[], []]
    everything = []

    def start(phase, stream):
        order = orders[stream]
        bit, left = order[phase], order[phase + 1 :]
        kept = subsets(left)
        flying[stream] = []
        for slot, subset in enumerate(kept):
            if phase == 0:
                block = flip(flip_all(me, subset), bit)
                source = grad_ref.at[block, pl.ds(stream * half, half)]
            else:
                source = sums[stream][phase - 1].at[len(kept) + slot]
            copy = pltpu.make_async_remote_copy(
                src_ref=source,
                dst_ref=gots[stream][phase].at[slot],
                send_sem=send_sem.at[stream, phase, slot],
                recv_sem=recv_sem.at[stream, phase, slot],
                device_id={"dp": flip(me, bit)},
                device_id_type=MESH,
            )
            copy.start()
            flying[stream].append(copy)
            everything.append(copy)

    def add(phase, stream):
        kept = subsets(orders[stream][phase + 1 :])
        for slot, subset in enumerate(kept):
            block = flip_all(me, subset)

            def step(i, carry):
                rows = pl.ds(pl.multiple_of(i * 16, 16), 16)
                if phase == 0:
                    begin = pl.multiple_of(stream * half + i * 16, 16)
                    mine = grad_ref[block, pl.ds(begin, 16)]
                else:
                    mine = sums[stream][phase - 1][slot, rows]
                came = gots[stream][phase][slot, rows]
                total = mine.astype(jnp.float32) + came.astype(jnp.float32)
                if phase == phases - 1:
                    out_ref[pl.ds(pl.multiple_of(stream * half + i * 16, 16), 16)] = total
                else:
                    sums[stream][phase][slot, rows] = total.astype(jnp.bfloat16)
                return carry

            lax.fori_loop(0, half // 16, step, 0)

    start(0, 0)
    start(0, 1)
    smalls = []
    for step in range(1, number):
        peer = lax.rem(me + step, number)
        copy = pltpu.make_async_remote_copy(
            src_ref=small_ref,
            dst_ref=gathered_ref.at[me],
            send_sem=small_send.at[step],
            recv_sem=small_recv.at[step],
            device_id={"dp": peer},
            device_id_type=MESH,
        )
        copy.start()
        smalls.append(copy)
    gathered_ref[me] = small_ref[...]
    for phase in range(phases):
        for stream in range(2):
            for copy in flying[stream]:
                copy.wait_recv()
            add(phase, stream)
            if phase < phases - 1:
                start(phase + 1, stream)
    for copy in everything:
        copy.wait_send()
    for copy in smalls:
        copy.wait()


def scatter_grad(mesh, grad, small, collective_id):
    number = mesh.shape["dp"]
    rows, width = grad.shape[0] // number, grad.shape[1]
    blocks = grad.reshape(number, rows, width)
    phases = number.bit_length() - 1
    gots = [
        pltpu.VMEM((number >> (phase + 1), rows // 2, width), jnp.bfloat16)
        for phase in range(phases)
    ]
    return pl.pallas_call(
        functools.partial(scatter_kernel, number),
        out_shape=[
            jax.ShapeDtypeStruct((rows, width), jnp.float32),
            jax.ShapeDtypeStruct((number,) + small.shape, small.dtype),
        ],
        in_specs=[pl.BlockSpec(memory_space=pltpu.VMEM)] * 2,
        out_specs=[pl.BlockSpec(memory_space=pltpu.VMEM)] * 2,
        scratch_shapes=gots
        + gots
        + gots[:-1]
        + gots[:-1]
        + [
            pltpu.SemaphoreType.DMA((2, phases, number // 2)),
            pltpu.SemaphoreType.DMA((2, phases, number // 2)),
            pltpu.SemaphoreType.DMA((number,)),
            pltpu.SemaphoreType.DMA((number,)),
        ],
        compiler_params=pltpu.CompilerParams(
            collective_id=collective_id, has_side_effects=True, vmem_limit_bytes=VMEM_BYTES
        ),
    )(blocks, small)


def gather_kernel(number, mine_ref, out_ref, local_sem, send_sem, recv_sem):
    me = lax.axis_index("dp")
    rows = mine_ref.shape[0]
    greet(("dp",), (number,), me, number)
    orders = [order[:0:-1] for order in bit_orders(number)]
    half = rows // 2
    local = pltpu.make_async_copy(mine_ref, out_ref.at[me], local_sem)
    local.start()
    copies = []
    held = [[[]], [[]]]
    slot = [0, 0]
    waiting = [[], []]
    across = []

    def send(stream, subset, bit):
        part = pl.ds(stream * half, half)
        block = flip_all(me, subset)
        copy = pltpu.make_async_remote_copy(
            src_ref=out_ref.at[block, part] if subset else mine_ref.at[part],
            dst_ref=out_ref.at[block, part],
            send_sem=send_sem.at[stream, slot[stream]],
            recv_sem=recv_sem.at[stream, slot[stream]],
            device_id={"dp": flip(me, bit)},
            device_id_type=MESH,
        )
        copy.start()
        copies.append(copy)
        slot[stream] += 1
        return copy

    fresh = [[[]], [[]]]
    for phase in range(len(orders[0]) + 1):
        for stream, order in enumerate(orders):
            for copy in waiting[stream]:
                copy.wait_recv()
            waiting[stream] = []
            if phase < len(order):
                bit = order[phase]
                waiting[stream] = [send(stream, subset, bit) for subset in held[stream]]
            across.extend(send(stream, subset, 0) for subset in fresh[stream])
            if phase < len(order):
                fresh[stream] = [subset + [bit] for subset in held[stream]]
                held[stream] = held[stream] + fresh[stream]
    for copy in across:
        copy.wait_recv()
    for copy in copies:
        copy.wait_send()
    local.wait()


def gather_weights(mesh, mine, collective_id):
    number = mesh.shape["dp"]
    out = pl.pallas_call(
        functools.partial(gather_kernel, number),
        out_shape=jax.ShapeDtypeStruct((number,) + mine.shape, mine.dtype),
        in_specs=[pl.BlockSpec(memory_space=pltpu.VMEM)],
        out_specs=pl.BlockSpec(memory_space=pltpu.VMEM),
        scratch_shapes=[
            pltpu.SemaphoreType.DMA,
            pltpu.SemaphoreType.DMA((2, number)),
            pltpu.SemaphoreType.DMA((2, number)),
        ],
        compiler_params=pltpu.CompilerParams(
            collective_id=collective_id, has_side_effects=True, vmem_limit_bytes=VMEM_BYTES
        ),
    )(mine)
    return out.reshape(number * mine.shape[0], mine.shape[1])


def pool_kernel(slab_ref, index_ref, out_ref, hot_ref, found_ref):
    slab = slab_ref[0]
    pairs, lanes = slab.shape
    batch, features = index_ref.shape[1:]
    pair_number = lax.broadcasted_iota(jnp.int32, (batch, pairs), 1)
    low = lax.broadcasted_iota(jnp.int32, (batch, lanes), 1) < lanes // 2
    for feature in range(features):
        column = index_ref[0, :, feature : feature + 1] >> 1
        hot_ref[pl.ds(feature * batch, batch), :] = jnp.where(
            column == pair_number, 1.0, 0.0
        ).astype(jnp.bfloat16)
    found_ref[...] = jnp.dot(hot_ref[...], slab, preferred_element_type=jnp.float32)
    for first in range(0, features, 2):
        halves = []
        for side in range(2):
            column = index_ref[0, :, first + side : first + side + 1]
            found = found_ref[pl.ds((first + side) * batch, batch), :]
            turned = pltpu.roll(found, lanes // 2, 1)
            halves.append(jnp.where((column & 1) == side, found, turned))
        start = first // 2 * lanes
        out_ref[:, start : start + lanes] = jnp.where(low, halves[0], halves[1]).astype(
            jnp.bfloat16
        )


def pool(slabs, indices):
    groups, pairs, lanes = slabs.shape
    batch, features = indices.shape[1:]
    return pl.pallas_call(
        pool_kernel,
        grid=(groups,),
        out_shape=jax.ShapeDtypeStruct((groups * batch, features * lanes // 2), jnp.bfloat16),
        in_specs=[
            pl.BlockSpec((1, pairs, lanes), lambda g: (g, 0, 0)),
            pl.BlockSpec((1, batch, features), lambda g: (g, 0, 0)),
        ],
        out_specs=pl.BlockSpec((batch, features * lanes // 2), lambda g: (g, 0)),
        scratch_shapes=[
            pltpu.VMEM((features * batch, pairs), jnp.bfloat16),
            pltpu.VMEM((features * batch, lanes), jnp.float32),
        ],
        compiler_params=pltpu.CompilerParams(vmem_limit_bytes=VMEM_BYTES),
    )(slabs, indices)


def slot_kernel(dact_ref, weight_ref, index_ref, turned_ref, out_ref, hot_ref, value_ref):
    pairs, lanes = out_ref.shape[1:]
    batch, features = index_ref.shape[1:]
    dpooled = lax.dot_general(
        dact_ref[...], weight_ref[...], (((1,), (1,)), ((), ())), preferred_element_type=jnp.float32
    )
    pair_number = lax.broadcasted_iota(jnp.int32, (pairs, batch), 0)
    upper = (lax.broadcasted_iota(jnp.int32, (batch, lanes), 1) >= lanes // 2).astype(jnp.int32)
    for feature in range(features):
        start = feature // 2 * lanes
        piece = dpooled[:, start : start + lanes]
        odd = index_ref[0, :, feature : feature + 1] & 1
        piece = jnp.where(odd == feature % 2, piece, pltpu.roll(piece, lanes // 2, 1))
        piece = jnp.where(upper == odd, piece, 0.0)
        high = piece.astype(jnp.bfloat16)
        rows = pl.ds(feature * batch, batch)
        value_ref[rows, 0:lanes] = high
        value_ref[rows, lanes : 2 * lanes] = (piece - high.astype(jnp.float32)).astype(jnp.bfloat16)
        line = turned_ref[0, feature : feature + 1, :] >> 1
        hot_ref[:, rows] = jnp.where(line == pair_number, 1.0, 0.0).astype(jnp.bfloat16)
    both = jnp.dot(hot_ref[...], value_ref[...], preferred_element_type=jnp.float32)
    out_ref[0] = (both[:, :lanes] + both[:, lanes:]).astype(jnp.bfloat16)


def slot_grads(dact, weight, indices, turned, pairs):
    groups, batch, features = indices.shape
    inputs, hidden = weight.shape
    lanes = 2 * inputs // features
    return pl.pallas_call(
        slot_kernel,
        grid=(groups,),
        out_shape=jax.ShapeDtypeStruct((groups, pairs, lanes), jnp.bfloat16),
        in_specs=[
            pl.BlockSpec((batch, hidden), lambda g: (g, 0)),
            pl.BlockSpec((inputs, hidden), lambda g: (0, 0)),
            pl.BlockSpec((1, batch, features), lambda g: (g, 0, 0)),
            pl.BlockSpec((1, features, batch), lambda g: (g, 0, 0)),
        ],
        out_specs=pl.BlockSpec((1, pairs, lanes), lambda g: (g, 0, 0)),
        scratch_shapes=[
            pltpu.VMEM((pairs, features * batch), jnp.bfloat16),
            pltpu.VMEM((features * batch, 2 * lanes), jnp.bfloat16),
        ],
        compiler_params=pltpu.CompilerParams(vmem_limit_bytes=VMEM_BYTES),
    )(dact, weight, indices, turned)


def table_kernel(arrived_ref, even_ref, odd_ref, out_ref):
    rows, width = out_ref.shape
    arrived = arrived_ref[...]
    count = arrived.shape[0]
    number = lax.broadcasted_iota(jnp.int32, (rows, count), 0) + pl.program_id(0) * rows
    even = jnp.where(even_ref[...] == number, 1.0, 0.0).astype(jnp.bfloat16)
    odd = jnp.where(odd_ref[...] == number, 1.0, 0.0).astype(jnp.bfloat16)
    first = jnp.dot(even, arrived, preferred_element_type=jnp.float32)
    second = jnp.dot(odd, arrived, preferred_element_type=jnp.float32)
    out_ref[...] = (first + pltpu.roll(second, width, 1))[:, :width]


def table_sums(arrived, even, odd, rows):
    count, lanes = arrived.shape
    tile = 512
    return pl.pallas_call(
        table_kernel,
        grid=(rows // tile,),
        out_shape=jax.ShapeDtypeStruct((rows, lanes // 2), jnp.float32),
        in_specs=[
            pl.BlockSpec((count, lanes), lambda r: (0, 0)),
            pl.BlockSpec((1, count), lambda r: (0, 0)),
            pl.BlockSpec((1, count), lambda r: (0, 0)),
        ],
        out_specs=pl.BlockSpec((tile, lanes // 2), lambda r: (r, 0)),
    )(arrived, even, odd)


def body(
    mesh,
    slab_values,
    row_ids,
    peer_counts,
    lookup_slots,
    labels,
    sample_weight,
    weight_in,
    bias_in,
    weight_out,
    dense_accum,
    table_rows,
    table_accum,
):
    peers = peer_counts.shape[1]
    capacity = row_ids.shape[2]
    emb_width = slab_values.shape[2] // capacity
    lanes = 2 * emb_width
    pairs = peers * capacity // 2
    index = slot_index(lookup_slots, peer_counts[0], capacity)
    slabs, turned = exchange(
        mesh, ("mp",), (slab_values.reshape(pairs, lanes), index.T), (False, False), 0
    )
    indices = jnp.swapaxes(turned, 1, 2)
    group = pool(slabs, indices)
    act = jnp.dot(group, weight_in, preferred_element_type=jnp.float32) + bias_in
    hidden = jax.nn.silu(act).astype(jnp.bfloat16)
    logit_part = jnp.dot(hidden, weight_out, preferred_element_type=jnp.float32)
    (logit_parts,) = exchange(mesh, ("mp",), (logit_part.reshape(-1, 128),), (False,), 1)
    logit = jnp.sum(logit_parts, axis=0).reshape(-1)
    dlogit = sample_weight * (jax.nn.sigmoid(logit) - labels.astype(jnp.float32))
    sigma = jax.nn.sigmoid(act)
    dact = (
        dlogit[:, None]
        * weight_out.astype(jnp.float32)[None, :]
        * sigma
        * (1.0 + act * (1.0 - sigma))
    ).astype(jnp.bfloat16)
    grad_in = lax.dot_general(
        group, dact, (((0,), (0,)), ((), ())), preferred_element_type=jnp.float32
    ).astype(jnp.bfloat16)
    grad_bias = jnp.sum(dact.astype(jnp.float32), axis=0)
    grad_out = jnp.sum(dlogit[:, None] * hidden.astype(jnp.float32), axis=0)
    small = jnp.concatenate([grad_bias.reshape(-1, 128), grad_out.reshape(-1, 128)])
    grad_rows, smalls = scatter_grad(mesh, grad_in, small, 2)
    partial = slot_grads(dact, weight_in, indices, turned, pairs)
    (parts,) = exchange(mesh, ("mp",), (partial,), (True,), 3)
    slot_grad = jnp.sum(parts.astype(jnp.float32), axis=0)
    first_group = (lax.axis_index("dp") == 0).astype(jnp.float32)
    small_sum = jnp.sum(smalls, axis=0)
    square = (
        jnp.sum(grad_rows * grad_rows)
        + first_group * jnp.sum(small_sum * small_sum)
        + jnp.sum(slot_grad * slot_grad)
    )
    arrived, arrived_rows, squares = exchange(
        mesh,
        ("dp", "mp"),
        (
            slot_grad.astype(jnp.bfloat16).reshape(peers, capacity // 2, lanes),
            row_ids.reshape(peers, 1, capacity),
            jnp.full((8, 128), square, jnp.float32),
        ),
        (True, True, False),
        4,
    )
    total = jnp.sum(squares[:, 0, 0])
    scale = clip_norm / jnp.maximum(jnp.sqrt(total), clip_norm)
    own_rows = dense_accum.shape[0]
    row_start = lax.axis_index("dp") * own_rows
    clipped = scale * grad_rows
    accum_new = dense_accum + clipped * clipped
    weight_part = lax.dynamic_slice_in_dim(weight_in, row_start, own_rows, 0).astype(jnp.float32)
    updated = (weight_part - dense_rate * clipped / (jnp.sqrt(accum_new) + adagrad_eps)).astype(
        jnp.bfloat16
    )
    weight_new = gather_weights(mesh, updated, 5)
    flat_rows = arrived_rows.reshape(-1, 2)
    received = scale * table_sums(
        arrived.reshape(pairs, lanes),
        flat_rows[:, 0].reshape(1, -1),
        flat_rows[:, 1].reshape(1, -1),
        table_rows.shape[0],
    )
    table_accum_new = table_accum + jnp.mean(received * received, axis=1)
    table_new = table_rows - table_rate * received / (
        jnp.sqrt(table_accum_new)[:, None] + adagrad_eps
    )
    return (weight_new, accum_new, table_new, table_accum_new)


def solution(mesh):
    placed = (
        P(("dp", "mp"), None, None),
        P(("dp", "mp"), None, None),
        P(("dp", "mp"), None),
        P(("dp", "mp"), None),
        P("dp"),
        P("dp"),
        P(None, "mp"),
        P("mp"),
        P("mp"),
        P("dp", "mp"),
        P(("dp", "mp"), None),
        P(("dp", "mp")),
    )
    return jax.shard_map(
        functools.partial(body, mesh),
        mesh=mesh,
        in_specs=placed,
        out_specs=(P(None, "mp"), P("dp", "mp"), P(("dp", "mp"), None), P(("dp", "mp"))),
        check_vma=False,
    )
```
